32 devices in a mesh: cfg: 2 (over core), tm: 16 (over z, y, x).
Axes of the slice: x: 2, y: 2, z: 4, core: 2. Of those that a mesh axis runs over, the one named last changes fastest.
Arguments:
- queries: bfloat16 [2, 12288, 1152], P('cfg', 'tm'), may hold values from -6 to 6
- key_vectors: bfloat16 [2, 12288, 1152], P('cfg', 'tm'), may hold values from -12 to 12
- value_vectors: bfloat16 [2, 12288, 1152], P('cfg', 'tm'), may hold values from -4 to 4
- out_weight: bfloat16 [1152, 2240], replicated, may hold values from -0.1875 to 0.1875
- first_frame: int32 [32], P('tm'), may hold values from 0 to 31, as said below
Outputs:
- guided: bfloat16 [12288, 2240], P('tm', 'cfg')
The draws below stay inside these ranges and needn't reach their ends.
Inputs may be any that keep to these rules, and one draw needn't show every extreme that they name: first_frame[f] is 0 or lies between f - 4 and f; some frame f has first_frame[f] = f - 4.
All inputs are finite; a program needn't handle non-finite values.
Results may differ from the reference program's by a relative error of at most 0.014.
Values may be sent and summed in bfloat16 or wider, within the bound.
A program may use at most 192 MiB of HBM per device.

```python
import math
import jax
import jax.numpy as jnp
from jax import lax

D = 2240
H = 36
DH = 32
FR = 2
NEAR = 2
FT = 384
HD = 1152
NF = 32
TOKENS = 12288
WIN = 4


def shared_noise(key):
    noise_key = jax.random.fold_in(key, 11)
    return jnp.clip(jax.random.normal(noise_key, (2, NF, FT, H, DH), jnp.float32), -4.0, 4.0)


def draw_key_vectors(key, part):
    noise = shared_noise(key)
    scale_key = jax.random.fold_in(key, 13)
    lowest = 0.3
    scales = jnp.exp(jax.random.uniform(scale_key, (2, NF, 1, H, DH), jnp.float32, math.log(lowest), math.log(3.0)))
    return (noise * scales).reshape(2, NF * FT, H * DH).astype(jnp.bfloat16)


def draw_value_vectors(key, part):
    noise = shared_noise(key)
    mixing_key = jax.random.fold_in(key, 29)
    own_key = jax.random.fold_in(key, 23)
    offset_key = jax.random.fold_in(key, 27)
    mixing = jax.random.normal(mixing_key, (H, DH, DH), jnp.float32) / math.sqrt(DH)
    mixed = jnp.einsum('bgthd,hde->bgthe', noise, mixing)
    coupled = 0.9 * jnp.clip(mixed, -2.5, 2.5)
    own = 0.3 * jnp.clip(jax.random.normal(own_key, (2, NF, FT, H, DH), jnp.float32), -3.0, 3.0)
    offsets = jax.random.uniform(offset_key, (2, NF, 1, H, DH), jnp.float32, -0.8, 0.8)
    return (coupled + own + offsets).reshape(2, NF * FT, H * DH).astype(jnp.bfloat16)


def draw_first_frame(key, part):
    first_key = jax.random.fold_in(key, 31)
    second_key = jax.random.fold_in(key, 37)
    third_key = jax.random.fold_in(key, 41)
    frame_ids = jnp.arange(NF, dtype=jnp.int32)
    windowed = jax.random.randint(first_key, (NF,), 0, 2, dtype=jnp.int32)
    backward = jax.random.randint(second_key, (NF,), 0, WIN + 1, dtype=jnp.int32)
    starts = jnp.where(windowed == 1, jnp.maximum(frame_ids - backward, 0), 0)
    reaching = (frame_ids % FR == 0) & (frame_ids >= FR) & (frame_ids <= NEAR * FR)
    starts = jnp.where(reaching, 1, starts)
    chosen = jax.random.randint(third_key, (), WIN + 1, NF, dtype=jnp.int32)
    starts = jnp.where(frame_ids == chosen, frame_ids - WIN, starts)
    return starts.astype(jnp.int32)


def shard_levels(rng, dims, shards, low, high):
    factor_of = 1.0
    for dim, shards_of in shards:
        draws = jax.random.uniform(jax.random.fold_in(jax.random.fold_in(rng, 6), dim), (shards_of,), jnp.float32, low / len(shards), high / len(shards))
        factor_of = factor_of * jnp.repeat(jnp.exp(draws), dims[dim] // shards_of).reshape((-1,) + (1,) * (len(dims) - 1 - dim))
    return factor_of


def gaussian(stream_key, dims, spread, limit, split=(), held_as=jnp.bfloat16):
    array = spread * jax.random.normal(stream_key, dims, jnp.float32)
    if split:
        array = array * shard_levels(stream_key, dims, split, -0.22, 0.18)
    return jnp.clip(array, -limit, limit).astype(held_as)


def setup_inputs(seed: int = 0) -> dict:
    keys = jax.random.split(jax.random.key(seed), 6)
    return {
        "queries": gaussian(keys[0], (2, TOKENS, HD), 1.0, 6.0, ((0, 2), (1, 16))),
        "key_vectors": draw_key_vectors(jax.random.fold_in(keys[5], 71), 0),
        "value_vectors": draw_value_vectors(jax.random.fold_in(keys[5], 71), 0),
        "out_weight": gaussian(keys[3], (HD, D), HD ** -0.5, 0.1875),
        "first_frame": draw_first_frame(jax.random.fold_in(keys[5], 71), 0),
    }


guide_scale = 4.5
epsilon = 1e-6


def reference(queries, key_vectors, value_vectors, out_weight, first_frame):
    frame_ids = jnp.arange(NF, dtype=jnp.int32)
    starts = first_frame.astype(jnp.int32)
    results = []
    for branch in range(2):
        query_feats = jnp.maximum(queries[branch], 0).astype(jnp.float32).reshape(NF, FT, H, DH)
        key_feats = jnp.maximum(key_vectors[branch], 0).astype(jnp.float32).reshape(NF, FT, H, DH)
        value_feats = value_vectors[branch].astype(jnp.float32).reshape(NF, FT, H, DH)
        frame_states = jnp.einsum("gthd,gthe->ghde", key_feats, value_feats, precision=lax.Precision.HIGHEST)
        frame_sums = jnp.sum(key_feats, axis=1)
        cumulative_states = jnp.concatenate([jnp.zeros((1, H, DH, DH), jnp.float32), jnp.cumsum(frame_states, axis=0)], axis=0)
        cumulative_sums = jnp.concatenate([jnp.zeros((1, H, DH), jnp.float32), jnp.cumsum(frame_sums, axis=0)], axis=0)
        attended_states = cumulative_states[frame_ids + 1] - cumulative_states[starts]
        attended_sums = cumulative_sums[frame_ids + 1] - cumulative_sums[starts]
        numerator = jnp.einsum("gthd,ghde->gthe", query_feats, attended_states, precision=lax.Precision.HIGHEST)
        denominator = jnp.einsum("gthd,ghd->gth", query_feats, attended_sums, precision=lax.Precision.HIGHEST) + epsilon
        attended = (numerator / denominator[..., None]).astype(jnp.bfloat16).reshape(TOKENS, H * DH)
        results.append(jnp.dot(attended, out_weight, preferred_element_type=jnp.float32))
    return (results[1] + guide_scale * (results[0] - results[1])).astype(jnp.bfloat16)
```

```python
import functools

import jax
import jax.numpy as jnp
from jax import lax
from jax.experimental import pallas as pl
from jax.experimental.pallas import tpu as pltpu
from jax.sharding import PartitionSpec as P

DH = 32
NEAR = 2
LANES = 128
PER = LANES // DH
GROUP = 4
TILE = 256
PARTS = 2
SPLIT = (4, 3, 2)
VMEM_BYTES = 67043328

guide_scale = 4.5
epsilon = 1e-06


def head_mask(rows, block):
    row = lax.broadcasted_iota(jnp.int32, (rows, LANES), 0) // DH
    lane = lax.broadcasted_iota(jnp.int32, (rows, LANES), 1) // DH
    return lane == (block if rows == DH else row)


def flip(place, r):
    for bit in (1 << i for i in range(r.bit_length()) if r >> i & 1):
        place = place + bit * (1 - 2 * ((place // bit) % 2))
    return place


def group_spans(groups):
    spans, start = [], 0
    for size in SPLIT:
        stop = min(groups, start + size)
        spans.append((start, stop))
        start = stop
    spans[-1] = (spans[-1][0], groups)
    return spans


def project(wbuf, rows, sublanes):
    return lax.dot_general(
        wbuf[sublanes, :], rows, (((1,), (1,)), ((), ())),
        preferred_element_type=jnp.float32,
    ).astype(jnp.bfloat16)


def attend_kernel(
    n, gsize, ff_ref, q_ref, k_ref, v_ref, w_ref, comb, wbuf, obuf,
    kbuf, vbuf, qbuf, own_att, frames, near_out, near_in, tot_out, a_in, b_out, b_in, c_out, c_in, fin, other,
    load_sem, late_sem, a_sem, b_sem, c_sem, near_sem, q_sem, fin_sem, comb_sem,
):
    fr, height = frames.shape[:2]
    ft = kbuf.shape[0] // fr
    groups = kbuf.shape[1] // LANES
    base = groups * DH
    part = height // gsize
    me = lax.axis_index("tm")
    core = lax.axis_index("cfg")
    other_core = 1 - core
    place, level = me % gsize, me // gsize
    levels = n // gsize
    share = other.shape[0]
    mine, theirs = core * share, other_core * share

    loads = []
    for f in range(fr):
        rows = pl.ds(f * ft, ft)
        for which, (src, dst) in enumerate(((k_ref, kbuf), (v_ref, vbuf))):
            copy = pltpu.make_async_copy(src.at[rows], dst.at[rows], load_sem.at[2 * f + which])
            copy.start()
            loads.append(copy)

    def mate(r):
        return {"tm": me - place + (flip(place, r))}

    barrier = pltpu.get_barrier_semaphore()
    pl.semaphore_signal(barrier, inc=1, device_id={"cfg": other_core})
    count = jnp.int32(gsize)
    for r in range(1, gsize):
        pl.semaphore_signal(barrier, inc=1, device_id=mate(r))
    for steps in [gsize * d for d in range(1, levels)] + list(range(1, NEAR + 1)):
        @pl.when(me >= steps)
        def _():
            pl.semaphore_signal(barrier, inc=1, device_id={"tm": me - steps})

        count = count + jnp.where(me + steps < n, 1, 0)

    masks = [head_mask(DH, a) for a in range(PER)]
    for f in range(fr):
        loads[2 * f].wait()
        loads[2 * f + 1].wait()
        frames[f, base:, :] = jnp.zeros((height - base, LANES), jnp.float32)
        for g in range(groups):
            cols = slice(g * LANES, (g + 1) * LANES)
            keys = jnp.maximum(kbuf[f * ft:(f + 1) * ft, cols], 0)
            values = vbuf[f * ft:(f + 1) * ft, cols]
            full = lax.dot_general(
                values, keys, (((0,), (0,)), ((), ())), preferred_element_type=jnp.float32
            )
            compact = jnp.zeros((DH, LANES), jnp.float32)
            for a in range(PER):
                compact = jnp.where(masks[a], full[a * DH:(a + 1) * DH], compact)
            frames[f, g * DH:(g + 1) * DH, :] = compact
            frames[f, base + g:base + g + 1, :] = jnp.sum(
                keys.astype(jnp.float32), axis=0, keepdims=True
            )
    columns = wbuf.shape[0]
    own_rows = pl.ds(pl.multiple_of(mine * ft, LANES), share * ft)
    their_rows = pl.ds(pl.multiple_of(theirs * ft, LANES), share * ft)
    late = [
        pltpu.make_async_copy(q_ref.at[own_rows], qbuf.at[0], late_sem.at[0]),
        pltpu.make_async_copy(
            w_ref.at[pl.ds(pl.multiple_of(core * columns, 16), columns)],
            wbuf, late_sem.at[1],
        ),
    ]
    for copy in late:
        copy.start()
    total = frames[0]
    for f in range(1, fr):
        total = total + frames[f]
    tot_out[...] = total.astype(jnp.bfloat16)
    near_out[...] = frames[...].astype(jnp.bfloat16)
    own_part = pl.ds(pl.multiple_of(place * part, 16), part)
    a_in[place] = tot_out[own_part, :]
    for d in range(1, NEAR + 1):
        @pl.when(me < d)
        def _():
            near_in[d - 1] = jnp.zeros(near_in.shape[1:], jnp.bfloat16)
    for d in range(1, levels):
        @pl.when(level < d)
        def _():
            b_in[d - 1] = jnp.zeros(b_in.shape[1:], jnp.bfloat16)

    pl.semaphore_wait(barrier, count)

    def a_copy(r):
        return pltpu.make_async_remote_copy(
            src_ref=tot_out.at[pl.ds(pl.multiple_of((flip(place, r)) * part, 16), part)],
            dst_ref=a_in.at[place], send_sem=a_sem.at[0, r - 1], recv_sem=a_sem.at[1, r - 1],
            device_id=mate(r),
        )

    def b_copy(d):
        return pltpu.make_async_remote_copy(
            src_ref=b_out, dst_ref=b_in.at[d - 1], send_sem=b_sem.at[0, d - 1],
            recv_sem=b_sem.at[1, d - 1], device_id={"tm": me + d * gsize},
        )

    def c_copy(r):
        return pltpu.make_async_remote_copy(
            src_ref=c_out.at[flip(place, r)], dst_ref=c_in.at[place], send_sem=c_sem.at[0, r - 1],
            recv_sem=c_sem.at[1, r - 1], device_id=mate(r),
        )

    def near_copy(d):
        return pltpu.make_async_remote_copy(
            src_ref=near_out, dst_ref=near_in.at[d - 1], send_sem=near_sem.at[0, d - 1],
            recv_sem=near_sem.at[1, d - 1], device_id={"tm": me + d},
        )

    q_copy = pltpu.make_async_remote_copy(
        src_ref=q_ref.at[their_rows], dst_ref=qbuf.at[1], send_sem=q_sem.at[0], recv_sem=q_sem.at[1],
        device_id={"cfg": other_core},
    )
    for r in reversed(range(1, gsize)):
        a_copy(r).start()
    for d in reversed(range(1, NEAR + 1)):
        @pl.when(me + d < n)
        def _():
            near_copy(d).start()
    q_copy.start()

    for r in range(1, gsize):
        a_copy(r).wait_recv()
    before = [jnp.zeros((part, LANES), jnp.float32)]
    for k in range(gsize):
        before.append(before[-1] + a_in[k].astype(jnp.float32))
    b_out[...] = before[-1].astype(jnp.bfloat16)
    for d in reversed(range(1, levels)):
        @pl.when(level + d < levels)
        def _():
            b_copy(d).start()
    for d in range(1, levels):
        @pl.when(level >= d)
        def _():
            b_copy(d).wait_recv()
    lower = jnp.zeros((part, LANES), jnp.float32)
    for d in range(1, levels):
        lower = lower + b_in[d - 1].astype(jnp.float32)
    for k in range(gsize):
        c_out[k] = (lower + before[k]).astype(jnp.bfloat16)
    for r in reversed(range(1, gsize)):
        c_copy(r).start()
    c_in[place] = c_out[place]
    for d in reversed(range(1, NEAR + 1)):
        @pl.when(me >= d)
        def _():
            near_copy(d).wait_recv()
    for r in range(1, gsize):
        c_copy(r).wait_recv()

    for j in range(fr):
        first = ff_ref[j]
        whole = first == 0
        acc = jnp.where(whole, 1.0, 0.0) * jnp.concatenate(
            [c_in[k].astype(jnp.float32) for k in range(gsize)], axis=0
        )
        for f in range(j + 1):
            acc = acc + jnp.where(me * fr + f >= first, 1.0, 0.0) * frames[f]
        for d in range(1, NEAR + 1):
            for f in range(fr):
                inside = jnp.logical_and(first > 0, (me - d) * fr + f >= first)
                acc = acc + jnp.where(inside, 1.0, 0.0) * near_in[d - 1, f].astype(jnp.float32)
        fin[j] = acc
    fin_copy = pltpu.make_async_remote_copy(
        src_ref=fin.at[pl.ds(theirs, share)], dst_ref=other, send_sem=fin_sem.at[0], recv_sem=fin_sem.at[1],
        device_id={"cfg": other_core},
    )
    fin_copy.start()

    own_scale = jnp.where(core == 0, guide_scale, 1.0 - guide_scale)
    other_scale = 1.0 - own_scale
    diagonal = head_mask(LANES, 0)

    def attended(b, source, f, i, g):
        compact = source[f, g * DH:(g + 1) * DH, :]
        sums = source[f, base + g:base + g + 1, :]
        state = jnp.where(diagonal, jnp.concatenate([compact] * PER, axis=0), 0.0)
        total = jnp.where(diagonal, jnp.broadcast_to(sums, (LANES, LANES)), 0.0)
        both = jnp.concatenate([state, total], axis=0)
        upper = both.astype(jnp.bfloat16)
        lower = (both - upper.astype(jnp.float32)).astype(jnp.bfloat16)
        feats = jnp.maximum(qbuf[b, i * ft:(i + 1) * ft, g * LANES:(g + 1) * LANES], 0)
        both = lax.dot_general(
            jnp.concatenate([feats, feats], axis=1),
            jnp.concatenate([upper, lower], axis=1),
            (((1,), (1,)), ((), ())), preferred_element_type=jnp.float32,
        )
        return both[:, :LANES] / (both[:, LANES:] + epsilon)

    late[0].wait()
    for i in range(share):
        for g in range(groups):
            own_att[i * ft:(i + 1) * ft, g * LANES:(g + 1) * LANES] = own_scale * attended(0, fin, mine + i, i, g)
    fin_copy.wait_recv()
    q_copy.wait_recv()
    comb_copies = []
    for s, (start, stop) in enumerate(group_spans(groups)):
        for g in range(start, stop):
            cols = slice(g * LANES, (g + 1) * LANES)
            for i in range(share):
                value = own_att[i * ft:(i + 1) * ft, cols] + other_scale * attended(1, other, i, i, g)
                comb[pl.ds(pl.multiple_of((mine + i) * ft, LANES), ft), cols] = value.astype(jnp.bfloat16)
        block = comb.at[own_rows, pl.ds(start * LANES, (stop - start) * LANES)]
        copy = pltpu.make_async_remote_copy(
            src_ref=block, dst_ref=block, send_sem=comb_sem.at[0, s], recv_sem=comb_sem.at[1, s],
            device_id={"cfg": other_core},
        )
        copy.start()
        comb_copies.append(copy)
    late[1].wait()
    rows = comb.shape[0]
    tile = pl.ds(pl.multiple_of(core * (rows - TILE), LANES), TILE)
    obuf[...] = project(wbuf, comb[tile, :], slice(0, columns))
    for copy in comb_copies:
        copy.wait()
    fin_copy.wait_send()
    q_copy.wait_send()
    for r in range(1, gsize):
        a_copy(r).wait_send()
        c_copy(r).wait_send()
    for d in range(1, levels):
        @pl.when(level + d < levels)
        def _():
            b_copy(d).wait_send()
    for d in range(1, NEAR + 1):
        @pl.when(me + d < n)
        def _():
            near_copy(d).wait_send()


def project_kernel(comb, wbuf, first, o_ref, obuf, sems):

    columns, rows = obuf.shape
    core = lax.axis_index("cfg")
    tile = TILE
    near = core * (rows - tile)
    far = (1 - core) * (rows - tile)
    span = pl.ds(pl.multiple_of(near, LANES), tile)
    copies = [pltpu.make_async_copy(first, o_ref.at[:, span], sems.at[0])]
    copies[0].start()
    starts = [tile * t for t in range(1, rows // tile - 1)] + [pl.multiple_of(far, LANES)]
    height = columns // PARTS
    for t, start in enumerate(starts):
        for h in range(PARTS):
            part = slice(h * height, (h + 1) * height)
            cols = pl.ds(start, tile)
            obuf[part, cols] = project(wbuf, comb[cols, :], part)
            copy = pltpu.make_async_copy(
                obuf.at[pl.ds(h * height, height), cols], o_ref.at[pl.ds(h * height, height), cols],
                sems.at[1 + t * PARTS + h],
            )
            copy.start()
            copies.append(copy)
    for copy in copies:
        copy.wait()


def on_device(n, cores, queries, key_vectors, value_vectors, out_weight, first_frame):
    rows, width = queries.shape[1:]
    fr = first_frame.shape[0]
    groups = width // LANES
    gsize = min(GROUP, n)
    levels = n // gsize
    height = groups * DH + groups
    height += -height % (16 * gsize)
    part = height // gsize
    share = fr // cores
    ft = rows // fr
    flat = lambda a: a.reshape(rows, width)
    f32, bf16 = jnp.float32, jnp.bfloat16
    hbm = pl.BlockSpec(memory_space=pltpu.HBM)
    vmem = pl.BlockSpec(memory_space=pltpu.VMEM)
    columns = out_weight.shape[1] // cores
    far = max(levels - 1, 1)
    dma = pltpu.SemaphoreType.DMA
    handed = 2 * (rows * width + columns * width + columns * TILE)
    comb, wbuf, obuf = pl.pallas_call(
        functools.partial(attend_kernel, n, gsize),
        name="attend",
        out_shape=[
            pltpu.VMEM((rows, width), bf16),
            pltpu.VMEM((columns, width), bf16),
            pltpu.VMEM((columns, TILE), bf16),
        ],
        in_specs=[pl.BlockSpec(memory_space=pltpu.SMEM), hbm, hbm, hbm, hbm],
        out_specs=[vmem] * 3,
        scratch_shapes=[
            pltpu.VMEM((rows, width), bf16),
            pltpu.VMEM((rows, width), bf16),
            pltpu.VMEM((2, share * ft, width), bf16),
            pltpu.VMEM((share * ft, width), f32),
            pltpu.VMEM((fr, height, LANES), f32),
            pltpu.VMEM((fr, height, LANES), bf16),
            pltpu.VMEM((NEAR, fr, height, LANES), bf16),
            pltpu.VMEM((height, LANES), bf16),
            pltpu.VMEM((gsize, part, LANES), bf16),
            pltpu.VMEM((part, LANES), bf16),
            pltpu.VMEM((far, part, LANES), bf16),
            pltpu.VMEM((gsize, part, LANES), bf16),
            pltpu.VMEM((gsize, part, LANES), bf16),
            pltpu.VMEM((fr, height, LANES), f32),
            pltpu.VMEM((share, height, LANES), f32),
            dma((2 * fr,)),
            dma((2,)),
            dma((2, gsize - 1)),
            dma((2, far)),
            dma((2, gsize - 1)),
            dma((2, NEAR)),
            dma((2,)),
            dma((2,)),
            dma((2, len(SPLIT))),
        ],
        compiler_params=pltpu.CompilerParams(
            collective_id=0, has_side_effects=True, vmem_limit_bytes=VMEM_BYTES - handed
        ),
    )(first_frame, flat(queries), flat(key_vectors), flat(value_vectors), out_weight.T)
    flipped = pl.pallas_call(
        project_kernel,
        name="project",
        out_shape=jax.ShapeDtypeStruct((columns, rows), bf16),
        in_specs=[vmem] * 3,
        out_specs=hbm,
        scratch_shapes=[
            pltpu.VMEM((columns, rows), bf16),
            dma((1 + PARTS * (rows // TILE),)),
        ],
        compiler_params=pltpu.CompilerParams(vmem_limit_bytes=40 * 2**20),
    )(comb, wbuf, obuf)
    return flipped.T


def solution(mesh):
    placed = (P("cfg", "tm", None), P("cfg", "tm", None), P("cfg", "tm", None), P(), P("tm"))
    return jax.shard_map(
        functools.partial(on_device, mesh.shape["tm"], mesh.shape["cfg"]),
        mesh=mesh, in_specs=placed, out_specs=P("tm", "cfg"), check_vma=False,
    )
```
